32 devices in a mesh: tm: 8 (over y, x, core), batch: 4 (over z).
Axes of the slice: x: 2, y: 2, z: 4, core: 2. Of those that a mesh axis runs over, the one named last changes fastest.
Arguments:
- hidden_states: bfloat16 [4, 1024, 5120], P('batch', 'tm'), may hold values from -6 to 6
- gen_weight: bfloat16 [64, 5120], replicated, may hold values from -0.078125 to 0.078125
- noise_field: bfloat16 [4, 64, 1024], P('batch', None, 'tm'), may hold values from -6 to 6
- timesteps: int32 [4], P('batch'), may hold values from 200 to 999
- embed_real: bfloat16 [128, 5120], replicated, may hold values from -0.5 to 0.5
- time_real: bfloat16 [256, 3, 5120], P('tm'), may hold values from -0.375 to 0.375
- query_real: bfloat16 [5120, 1024], P(None, 'tm'), may hold values from -3 to 3
- key_real: bfloat16 [5120, 1024], P(None, 'tm'), may hold values from -3 to 3
- value_real: bfloat16 [5120, 1024], P(None, 'tm'), may hold values from -0.078125 to 0.078125
- out_real: bfloat16 [1024, 5120], P('tm'), may hold values from -0.1875 to 0.1875
- gain_real: float32 [2, 1024], P(None, 'tm'), may hold values from 0.25 to 3
- proj_real: bfloat16 [64, 5120], replicated, may hold values from -0.078125 to 0.078125
- embed_fake: bfloat16 [128, 5120], replicated, may hold values from -0.5 to 0.5
- time_fake: bfloat16 [256, 3, 5120], P('tm'), may hold values from -0.375 to 0.375
- query_fake: bfloat16 [5120, 1024], P(None, 'tm'), may hold values from -3 to 3
- key_fake: bfloat16 [5120, 1024], P(None, 'tm'), may hold values from -3 to 3
- value_fake: bfloat16 [5120, 1024], P(None, 'tm'), may hold values from -0.078125 to 0.078125
- out_fake: bfloat16 [1024, 5120], P('tm'), may hold values from -0.1875 to 0.1875
- gain_fake: float32 [2, 1024], P(None, 'tm'), may hold values from 0.25 to 3
- proj_fake: bfloat16 [64, 5120], replicated, may hold values from -0.078125 to 0.078125
Outputs:
- dmd_gradient: float32 [4, 64, 1024], P('batch', None, 'tm')
- weight_grad: float32 [64, 5120], replicated
The draws below stay inside these ranges and needn't reach their ends.
All inputs are finite; a program needn't handle non-finite values.
Results may differ from the reference program's by a relative error of at most 0.019.
Values may be sent and summed in bfloat16 or wider, within the bound.
A program may use at most 128 MiB of HBM per device.

```python
import math
import jax
import jax.numpy as jnp
from jax import lax

D = 5120
HD = 128
FREQ = 256
FTOK = 128
HEADS = 8
PATCH = 64
KIN = 128
TOKENS = 1024
SAMPLES = 4


def spiked_pair(key, salt_value):
    base_key = jax.random.fold_in(key, salt_value)
    key_one, key_two, key_three, key_four = jax.random.split(base_key, 4)
    proj_width = HEADS * HD
    query_draw = jax.random.normal(key_one, (D, proj_width), jnp.float32) / math.sqrt(D)
    key_draw = jax.random.normal(key_four, (D, proj_width), jnp.float32) / math.sqrt(D)
    return (jnp.clip(query_draw, -3.0, 3.0), jnp.clip(key_draw, -3.0, 3.0))


def draw_query_real(key, part):
    return spiked_pair(key, 11)[0].astype(jnp.bfloat16)


def draw_key_real(key, part):
    return spiked_pair(key, 11)[1].astype(jnp.bfloat16)


def draw_query_fake(key, part):
    return spiked_pair(key, 23)[0].astype(jnp.bfloat16)


def draw_key_fake(key, part):
    return spiked_pair(key, 23)[1].astype(jnp.bfloat16)


def touch_ends(drawn, key, smallest, largest):
    longest = drawn.shape.index(max(drawn.shape))
    spots = []
    for shift in (0, 1):
        where = [jax.random.randint(jax.random.fold_in(key, axis), (), 0, length) for axis, length in enumerate(drawn.shape)]
        where[longest] = (where[longest] + shift) % drawn.shape[longest]
        spots.append(tuple(where))
    return drawn.at[spots[0]].set(smallest).at[spots[1]].set(largest)


def level_of(key, extent, shards, low, top_value):
    def one(position, parts):
        steps = jax.random.uniform(jax.random.fold_in(jax.random.fold_in(key, 6), position), (parts,), jnp.float32, low / len(shards), top_value / len(shards))
        return jnp.repeat(jnp.exp(steps), extent[position] // parts).reshape((-1,) + (1,) * (len(extent) - position - 1))

    factor_of = one(*shards[0])
    for cut in shards[1:]:
        factor_of = factor_of * one(*cut)
    return factor_of


def scatter_about(rng, dims, deviation, most, cuts=(), kind=jnp.bfloat16):
    factor_of = level_of(rng, dims, cuts, -0.22, 0.18) if cuts else 1.0
    values = jax.random.normal(rng, dims, jnp.float32) * deviation * factor_of
    return jnp.minimum(jnp.maximum(values, -most), most).astype(kind)


def setup_inputs(seed: int = 0) -> dict:
    seeds = jax.random.split(jax.random.key(seed), 21)
    hidden_states = scatter_about(seeds[0], (SAMPLES, TOKENS, D), 1.0, 6.0, ((0, 4), (1, 8)))
    gen_weight = scatter_about(seeds[1], (PATCH, D), D ** -0.5, 0.078125)
    noise_field = scatter_about(seeds[2], (SAMPLES, PATCH, TOKENS), 1.0, 6.0, ((0, 4), (2, 8)))
    timesteps = touch_ends(jax.random.randint(seeds[3], (SAMPLES,), 200, 1000), jax.random.fold_in(seeds[3], 1), 200, 999).astype(jnp.int32)
    embed_real = scatter_about(seeds[4], (KIN, D), KIN ** -0.5, 0.5)
    time_real = scatter_about(seeds[5], (FREQ, 3, D), FREQ ** -0.5, 0.375, ((0, 8),))
    query_real = draw_query_real(jax.random.fold_in(seeds[20], 71), 0)
    key_real = draw_key_real(jax.random.fold_in(seeds[20], 71), 0)
    value_real = scatter_about(seeds[8], (D, HEADS * HD), D ** -0.5, 0.078125, ((1, 8),))
    out_real = scatter_about(seeds[9], (HEADS * HD, D), (HEADS * HD) ** -0.5, 0.1875, ((0, 8),))
    gain_real = jnp.clip(jnp.exp(math.log(3.0) - 2.4849066 * jax.random.uniform(seeds[10], (2, HEADS * HD), jnp.float32) ** level_of(seeds[10], (2, HEADS * HD), ((1, 8),), -0.2, 0.2)), 0.25, 3.0)
    proj_real = scatter_about(seeds[11], (PATCH, D), D ** -0.5, 0.078125)
    embed_fake = scatter_about(seeds[12], (KIN, D), KIN ** -0.5, 0.5)
    time_fake = scatter_about(seeds[13], (FREQ, 3, D), FREQ ** -0.5, 0.375, ((0, 8),))
    query_fake = draw_query_fake(jax.random.fold_in(seeds[20], 71), 0)
    key_fake = draw_key_fake(jax.random.fold_in(seeds[20], 71), 0)
    value_fake = scatter_about(seeds[16], (D, HEADS * HD), D ** -0.5, 0.078125, ((1, 8),))
    out_fake = scatter_about(seeds[17], (HEADS * HD, D), (HEADS * HD) ** -0.5, 0.1875, ((0, 8),))
    gain_fake = jnp.clip(jnp.exp(math.log(3.0) - 2.4849066 * jax.random.uniform(seeds[18], (2, HEADS * HD), jnp.float32) ** level_of(seeds[18], (2, HEADS * HD), ((1, 8),), -0.2, 0.2)), 0.25, 3.0)
    proj_fake = scatter_about(seeds[19], (PATCH, D), D ** -0.5, 0.078125)
    return dict(hidden_states=hidden_states, gen_weight=gen_weight, noise_field=noise_field, timesteps=timesteps, embed_real=embed_real, time_real=time_real, query_real=query_real, key_real=key_real, value_real=value_real, out_real=out_real, gain_real=gain_real, proj_real=proj_real, embed_fake=embed_fake, time_fake=time_fake, query_fake=query_fake, key_fake=key_fake, value_fake=value_fake, out_fake=out_fake, gain_fake=gain_fake, proj_fake=proj_fake)


norm_floor = 0.05
gap_floor = 0.25
highest = lax.Precision.HIGHEST

def sinusoid(time_step):
    half_freq = FREQ // 2
    frequency = jnp.exp(-math.log(10000.0) * jnp.arange(half_freq, dtype=jnp.float32) / half_freq)
    angles = time_step.astype(jnp.float32) * frequency
    return jnp.concatenate([jnp.cos(angles), jnp.sin(angles)]).astype(jnp.bfloat16)

def rms_round(vector, gain_row):
    return (vector * lax.rsqrt(lax.optimization_barrier(jnp.mean(vector * vector, axis=1, keepdims=True)) + norm_floor) * gain_row[None, :]).astype(jnp.bfloat16)

def velocity(noisy_patch, sinus_wave, embed_table, time_table, query_proj, key_proj, value_proj, out_proj, norm_gains, final_proj):
    earlier = jnp.concatenate([jnp.zeros((PATCH, FTOK), jnp.bfloat16), noisy_patch[:, :TOKENS - FTOK]], axis=1)
    stacked = jnp.concatenate([noisy_patch, earlier], axis=0)
    embedded = lax.dot_general(stacked, embed_table, (((0,), (0,)), ((), ())), preferred_element_type=jnp.float32)
    row_mean = lax.optimization_barrier(jnp.mean(embedded, axis=1, keepdims=True))
    centered = embedded - row_mean
    rscale = lax.rsqrt(lax.optimization_barrier(jnp.mean(centered * centered, axis=1, keepdims=True)) + norm_floor)
    modulation = jnp.einsum('f,fcd->cd', sinus_wave.astype(jnp.float32), time_table.astype(jnp.float32))
    normed = centered * rscale * (1.0 + modulation[1])[None, :] + modulation[0][None, :]
    queries = jnp.dot(normed, query_proj.astype(jnp.float32), precision=highest)
    keys_all = jnp.dot(normed, key_proj.astype(jnp.float32), precision=highest)
    values_all = jnp.dot(normed, value_proj.astype(jnp.float32), precision=highest).astype(jnp.bfloat16)
    query_norm = rms_round(queries, norm_gains[0])
    key_norm = rms_round(keys_all, norm_gains[1])
    frames = jnp.arange(TOKENS, dtype=jnp.int32) // FTOK
    allowed = frames[None, :] <= frames[:, None]

    def one_head(head_index):
        start_col = head_index * HD
        query_head = lax.dynamic_slice_in_dim(query_norm, start_col, HD, 1)
        key_head = lax.dynamic_slice_in_dim(key_norm, start_col, HD, 1)
        value_head = lax.dynamic_slice_in_dim(values_all, start_col, HD, 1)
        scores = jnp.dot(query_head, key_head.T, preferred_element_type=jnp.float32) / math.sqrt(HD)
        scores = jnp.where(allowed, scores, -1e+30)
        row_peak = lax.optimization_barrier(jnp.max(scores, axis=1, keepdims=True))
        exp_scores = jnp.exp(scores - row_peak)
        attn_probs = (exp_scores / lax.optimization_barrier(jnp.sum(exp_scores, axis=1, keepdims=True))).astype(jnp.bfloat16)
        return jnp.dot(attn_probs, value_head, preferred_element_type=jnp.float32).astype(jnp.bfloat16)
    per_head = lax.map(one_head, jnp.arange(HEADS, dtype=jnp.int32))
    attended = jnp.transpose(per_head, (1, 0, 2)).reshape(TOKENS, HEADS * HD)
    mixed = jnp.dot(attended, out_proj, preferred_element_type=jnp.float32)
    residual = embedded + mixed * modulation[2][None, :]
    return lax.dot_general(final_proj.astype(jnp.float32), residual, (((1,), (1,)), ((), ())), precision=highest)

def reference(hidden_states, gen_weight, noise_field, timesteps, embed_real, time_real, query_real, key_real, value_real, out_real, gain_real, proj_real, embed_fake, time_fake, query_fake, key_fake, value_fake, out_fake, gain_fake, proj_fake):
    grad_root = math.sqrt(SAMPLES * TOKENS)
    gradients = []
    grad_total = jnp.zeros((PATCH, D), jnp.float32)
    for sample in range(SAMPLES):
        time_step = timesteps[sample]
        level_raw = time_step.astype(jnp.float32) / 1000.0
        noise_level = 5.0 * level_raw / (1.0 + 4.0 * level_raw)
        generated = lax.dot_general(gen_weight, hidden_states[sample], (((1,), (1,)), ((), ())), preferred_element_type=jnp.float32).astype(jnp.bfloat16)
        noisy_patch = ((1.0 - noise_level) * generated.astype(jnp.float32) + noise_level * noise_field[sample].astype(jnp.float32)).astype(jnp.bfloat16)
        sinus_wave = sinusoid(time_step)
        vel_real = velocity(noisy_patch, sinus_wave, embed_real, time_real, query_real, key_real, value_real, out_real, gain_real, proj_real)
        vel_fake = velocity(noisy_patch, sinus_wave, embed_fake, time_fake, query_fake, key_fake, value_fake, out_fake, gain_fake, proj_fake)
        pred_real = noisy_patch.astype(jnp.float32) - noise_level * vel_real
        pred_fake = noisy_patch.astype(jnp.float32) - noise_level * vel_fake
        gap_mean = jnp.sum(jnp.abs(generated.astype(jnp.float32) - pred_real)) / (PATCH * TOKENS)
        normalizer = jnp.maximum(gap_mean, gap_floor)
        gap_diff = pred_fake - pred_real
        gradients.append(gap_diff / normalizer)
        difference = gap_diff.astype(jnp.bfloat16)
        partial_grad = jnp.dot(difference, hidden_states[sample], preferred_element_type=jnp.float32)
        grad_total = grad_total + partial_grad / normalizer / grad_root
    return (jnp.stack(gradients), grad_total)
```

```python
import functools
import math

import jax
import jax.numpy as jnp
from jax import lax
from jax.experimental import pallas as pl
from jax.experimental.pallas import tpu as pltpu
from jax.sharding import PartitionSpec as P

HD = 128
FREQ = 256
FTOK = 128


norm_floor = 0.05
gap_floor = 0.25
highest = lax.Precision.HIGHEST


MESH = pl.DeviceIdType.MESH
f32 = jnp.float32
bf16 = jnp.bfloat16


def greet(sizes):
    barrier = pltpu.get_barrier_semaphore()
    count = 0
    for axis, size in sizes.items():
        me = lax.axis_index(axis)
        for k in range(1, size):
            pl.semaphore_signal(
                barrier, inc=1, device_id={axis: lax.rem(me + k, size)}, device_id_type=MESH
            )
            count += 1
    pl.semaphore_wait(barrier, count)


def exchange(axis, size, source, slots, send, recv):
    me = lax.axis_index(axis)
    copies = []
    for k in range(1, size):
        peer = lax.rem(me + k, size)
        copy = pltpu.make_async_remote_copy(
            src_ref=source(peer),
            dst_ref=slots.at[me],
            send_sem=send.at[k],
            recv_sem=recv.at[k],
            device_id={axis: peer},
            device_id_type=MESH,
        )
        copy.start()
        copies.append(copy)
    return copies


def landed(copies):
    for copy in copies:
        copy.wait_recv()


def gone(copies):
    for copy in copies:
        copy.wait_send()


def sems(*sizes):
    return [pltpu.SemaphoreType.DMA((size,)) for size in sizes for _ in range(2)]


def comm_call(body, out_shape, scratch, collective_id, *args):
    vmem = pl.BlockSpec(memory_space=pltpu.VMEM)
    return pl.pallas_call(
        body,
        out_shape=out_shape,
        in_specs=[vmem] * len(args),
        out_specs=jax.tree.map(lambda _: vmem, out_shape),
        scratch_shapes=scratch,
        compiler_params=pltpu.CompilerParams(
            collective_id=collective_id, has_side_effects=True
        ),
    )(*args)


def start_kernel(n, noisy_ref, share_ref, patches_ref, modul_ref, parts, s1, r1, s2, r2, s3, r3):
    me = lax.axis_index("tm")
    greet({"tm": n})
    scatter = exchange("tm", n, lambda peer: share_ref.at[peer], parts, s1, r1)
    spread = exchange("tm", n, lambda peer: noisy_ref, patches_ref, s2, r2)
    patches_ref[me] = noisy_ref[...]
    parts[me] = share_ref[me]
    landed(scatter)
    modul_ref[me] = jnp.sum(parts[...], axis=0)
    collect = exchange("tm", n, lambda peer: modul_ref.at[me], modul_ref, s3, r3)
    landed(spread)
    landed(collect)
    gone(scatter)
    gone(spread)
    gone(collect)


def sums_kernel(n, own_ref, total_ref, parts, s1, r1):
    greet({"tm": n})
    spread = exchange("tm", n, lambda peer: own_ref, parts, s1, r1)
    parts[lax.axis_index("tm")] = own_ref[...]
    landed(spread)
    total_ref[...] = jnp.sum(parts[...], axis=0)
    gone(spread)


def terms_kernel(n, own_ref, total_ref, parts, s1, r1):
    me = lax.axis_index("tm")
    greet({"tm": n})
    scatter = exchange("tm", n, lambda peer: own_ref.at[peer], parts, s1, r1)
    parts[me] = own_ref[me]
    landed(scatter)
    total_ref[...] = jnp.sum(parts[...].astype(f32), axis=0)
    gone(scatter)


def grad_kernel(
    n, nb, count_all, grad_root, own_ref, gap_ref, grad_ref, norm_ref,
    parts, gaps, mixed, quarters, merged, s1, r1, s2, r2, s3, r3, s4, r4, s5, r5,
):
    me = lax.axis_index("tm")
    mine = lax.axis_index("batch")
    greet({"tm": n, "batch": nb})
    gap_copies = exchange("tm", n, lambda peer: gap_ref, gaps, s1, r1)
    scatter = exchange("tm", n, lambda peer: own_ref.at[peer], parts, s2, r2)
    gaps[me] = gap_ref[...]
    parts[me] = own_ref[me]
    landed(gap_copies)
    normalizer = jnp.maximum(jnp.sum(gaps[...], axis=0) / count_all, gap_floor)
    norm_ref[...] = normalizer
    landed(scatter)
    summed = jnp.sum(parts[...].astype(f32), axis=0) / normalizer[:1, :1] / grad_root
    mixed[...] = summed.reshape(mixed.shape).astype(bf16)
    across = exchange("batch", nb, lambda peer: mixed.at[peer], quarters, s3, r3)
    quarters[mine] = mixed[mine]
    landed(across)
    merged[mine] = jnp.sum(quarters[...].astype(f32), axis=0).astype(bf16)
    back = exchange("batch", nb, lambda peer: merged.at[mine], merged, s4, r4)
    landed(back)
    grad_ref[me] = merged[...]
    last = exchange("tm", n, lambda peer: merged, grad_ref, s5, r5)
    landed(last)
    for copies in (gap_copies, scatter, across, back, last):
        gone(copies)


def centered_table(embed_table):
    wide = embed_table.astype(f32)
    return wide - jnp.mean(wide, axis=1, keepdims=True)


def fold_heads(centered, modulation, weights):
    rows = jnp.concatenate([centered * (1.0 + modulation[1])[None, :], modulation[:1]], axis=0)
    high = rows.astype(bf16)
    low = (rows - high.astype(f32)).astype(bf16)
    both = jnp.concatenate([high, low], axis=0)
    folded = [jnp.dot(both, weight, preferred_element_type=f32) for weight in weights]
    folded = jnp.concatenate(folded, axis=1)
    return folded[: rows.shape[0]] + folded[rows.shape[0] :]


def project(stacked, gram, folded, width):
    kin_rows = stacked.shape[0]
    wide = stacked.astype(f32)
    variance = jnp.sum(wide * jnp.dot(gram, wide, precision=highest), axis=0)
    rscale = lax.rsqrt(jnp.maximum(variance, 0.0) + norm_floor)
    main = folded[:kin_rows]
    high = main.astype(bf16)
    low = (main - high.astype(f32)).astype(bf16)
    both = jnp.concatenate([high, low], axis=0)
    twice = jnp.concatenate([stacked, stacked], axis=0)
    base = lax.dot_general(
        twice, both, (((0,), (0,)), ((), ())), preferred_element_type=f32
    )
    full = rscale[:, None] * base + folded[kin_rows][None, :]
    return [full[:, i * width : (i + 1) * width] for i in range(3)]


def sinusoid(time_step):
    half_freq = FREQ // 2
    frequency = jnp.exp(-math.log(10000.0) * jnp.arange(half_freq, dtype=jnp.float32) / half_freq)
    angles = time_step.astype(jnp.float32) * frequency
    return jnp.concatenate([jnp.cos(angles), jnp.sin(angles)]).astype(jnp.bfloat16)


def rms_round(vector, total_sq, columns, gain_row):
    return (
        vector * lax.rsqrt(total_sq / columns + norm_floor)[:, None] * gain_row[None, :]
    ).astype(jnp.bfloat16)


def attend(query_norm, key_norm, value_norm):
    token_count = query_norm.shape[0]
    block_rows = min(512, token_count)
    frames = jnp.arange(token_count, dtype=jnp.int32) // FTOK

    def one_block(row_start):
        query_block = lax.dynamic_slice_in_dim(query_norm, row_start, block_rows, 0)
        scores = jnp.einsum(
            "qhd,khd->hqk", query_block, key_norm, preferred_element_type=jnp.float32
        ) / math.sqrt(HD)
        query_frames = lax.dynamic_slice_in_dim(frames, row_start, block_rows, 0)
        allowed = frames[None, :] <= query_frames[:, None]
        scores = jnp.where(allowed[None], scores, -1e30)
        row_peak = jnp.max(scores, axis=2, keepdims=True)
        exp_scores = jnp.exp(scores - row_peak)
        attn_probs = (exp_scores / jnp.sum(exp_scores, axis=2, keepdims=True)).astype(jnp.bfloat16)
        return jnp.einsum(
            "hqk,khd->qhd", attn_probs, value_norm, preferred_element_type=jnp.float32
        ).astype(jnp.bfloat16)

    starts = jnp.arange(token_count // block_rows, dtype=jnp.int32) * block_rows
    pieces = lax.map(one_block, starts)
    return pieces.reshape(token_count, query_norm.shape[1], query_norm.shape[2])


def per_device(
    hidden_states,
    gen_weight,
    noise_field,
    timesteps,
    embed_real,
    time_real,
    query_real,
    key_real,
    value_real,
    out_real,
    gain_real,
    proj_real,
    embed_fake,
    time_fake,
    query_fake,
    key_fake,
    value_fake,
    out_fake,
    gain_fake,
    proj_fake,
):
    devices = lax.axis_size("tm")
    frame_tokens = hidden_states.shape[1]
    tokens = frame_tokens * devices
    patch_rows = gen_weight.shape[0]
    time_step = timesteps[0]
    level_raw = time_step.astype(jnp.float32) / 1000.0
    noise_level = 5.0 * level_raw / (1.0 + 4.0 * level_raw)
    generated = lax.dot_general(
        gen_weight, hidden_states[0], (((1,), (1,)), ((), ())), preferred_element_type=f32
    ).astype(bf16)
    noisy_patch = (
        (1.0 - noise_level) * generated.astype(f32) + noise_level * noise_field[0].astype(f32)
    ).astype(bf16)
    sinus_wave = sinusoid(time_step)
    freq_rows = time_real.shape[0]
    own_wave = lax.dynamic_slice_in_dim(sinus_wave, lax.axis_index("tm") * freq_rows, freq_rows, 0)
    model_width = hidden_states.shape[2]
    part_width = model_width // devices
    shares = jnp.concatenate(
        [
            jnp.dot(own_wave[None], t.reshape(freq_rows, -1), preferred_element_type=f32).reshape(
                3, devices, part_width
            )
            for t in (time_real, time_fake)
        ]
    ).transpose(1, 0, 2)
    patches, modul = comm_call(
        functools.partial(start_kernel, devices),
        [
            jax.ShapeDtypeStruct((devices, patch_rows, frame_tokens), bf16),
            jax.ShapeDtypeStruct((devices, 6, part_width), f32),
        ],
        [pltpu.VMEM((devices, 6, part_width), f32), *sems(devices, devices, devices)],
        0,
        noisy_patch,
        shares,
    )
    modul = modul.transpose(1, 0, 2).reshape(6, model_width)
    all_patch = patches.transpose(1, 0, 2).reshape(patch_rows, tokens)
    prior_frame = jnp.pad(all_patch, ((0, 0), (frame_tokens, 0)))[:, :tokens]
    all_stacked = jnp.concatenate([all_patch, prior_frame], axis=0)
    local_width = query_real.shape[1]
    local_heads = local_width // HD
    columns = local_width * devices
    qkv = []
    embeds = []
    nets = (
        (embed_real, modul[:3], query_real, key_real, value_real, gain_real, out_real, proj_real),
        (embed_fake, modul[3:], query_fake, key_fake, value_fake, gain_fake, out_fake, proj_fake),
    )
    own_stacked = lax.dynamic_slice_in_dim(
        all_stacked, lax.axis_index("tm") * frame_tokens, frame_tokens, 1
    )
    direct = []
    for embed, modulation, query, key, value, _, _, proj in nets:
        centered = centered_table(embed)
        gram = jnp.dot(centered, centered.T, precision=lax.Precision.HIGH) / model_width
        folded = fold_heads(centered, modulation, (query, key, value))
        qkv.append(project(all_stacked, gram, folded, local_width))
        inner = lax.dot_general(
            proj, embed, (((1,), (1,)), ((), ())), preferred_element_type=f32
        )
        direct.append(jnp.dot(inner, own_stacked.astype(f32), precision=highest))
    squares = jnp.stack([jnp.sum(qkv[i][j] * qkv[i][j], axis=1) for i in (0, 1) for j in (0, 1)])
    norm_sums = comm_call(
        functools.partial(sums_kernel, devices),
        jax.ShapeDtypeStruct((4, tokens), f32),
        [pltpu.VMEM((devices, 4, tokens), f32), *sems(devices)],
        1,
        squares,
    )
    head_shape = (tokens, local_heads, HD)
    terms = []
    for i, (_, modulation, _, _, _, gain, out, proj) in enumerate(nets):
        attended = attend(
            rms_round(qkv[i][0], norm_sums[2 * i], columns, gain[0]).reshape(head_shape),
            rms_round(qkv[i][1], norm_sums[2 * i + 1], columns, gain[1]).reshape(head_shape),
            qkv[i][2].astype(bf16).reshape(head_shape),
        ).reshape(devices, frame_tokens, local_width)
        gated = proj.astype(f32) * modulation[2][None, :]
        high = gated.astype(bf16)
        low = (gated - high.astype(f32)).astype(bf16)
        folded_out = lax.dot_general(
            jnp.concatenate([high, low], axis=0), out, (((1,), (1,)), ((), ())),
            preferred_element_type=f32,
        )
        folded_out = folded_out[:patch_rows] + folded_out[patch_rows:]
        terms.append(
            jnp.einsum("rc,ntc->nrt", folded_out.astype(bf16), attended, preferred_element_type=f32)
        )
    own_terms = comm_call(
        functools.partial(terms_kernel, devices),
        jax.ShapeDtypeStruct((2 * patch_rows, frame_tokens), f32),
        [pltpu.VMEM((devices, 2 * patch_rows, frame_tokens), bf16), *sems(devices)],
        2,
        jnp.concatenate(terms, axis=1).astype(bf16),
    )
    velocity_real = own_terms[:patch_rows] + direct[0]
    velocity_fake = own_terms[patch_rows:] + direct[1]
    pred_real = noisy_patch.astype(f32) - noise_level * velocity_real
    pred_fake = noisy_patch.astype(f32) - noise_level * velocity_fake
    gap_local = jnp.sum(jnp.abs(generated.astype(f32) - pred_real))
    count_all = patch_rows * tokens
    batches = lax.axis_size("batch")
    grad_root = math.sqrt(batches * hidden_states.shape[0] * tokens)
    gap_diff = pred_fake - pred_real
    difference = gap_diff.astype(bf16)
    partial_grad = jnp.dot(difference, hidden_states[0], preferred_element_type=f32)
    partial_grad = partial_grad.astype(bf16).reshape(patch_rows, devices, part_width)
    quarter = patch_rows // batches
    piece = (batches, quarter, part_width)
    grad, norm = comm_call(
        functools.partial(grad_kernel, devices, batches, count_all, grad_root),
        [
            jax.ShapeDtypeStruct((devices, *piece), bf16),
            jax.ShapeDtypeStruct((8, 128), f32),
        ],
        [
            pltpu.VMEM((devices, patch_rows, part_width), bf16),
            pltpu.VMEM((devices, 8, 128), f32),
            pltpu.VMEM(piece, bf16),
            pltpu.VMEM(piece, bf16),
            pltpu.VMEM(piece, bf16),
            *sems(devices, devices, batches, batches, devices),
        ],
        3,
        partial_grad.transpose(1, 0, 2),
        jnp.broadcast_to(gap_local, (8, 128)),
    )
    weight_grad = grad.reshape(devices, patch_rows, part_width).transpose(1, 0, 2)
    weight_grad = weight_grad.reshape(patch_rows, model_width).astype(f32)
    dmd_gradient = (gap_diff / norm[0, 0])[None]
    return (dmd_gradient, weight_grad)


def solution(mesh):
    in_specs = (
        P("batch", "tm", None),
        P(),
        P("batch", None, "tm"),
        P("batch"),
        P(),
        P("tm", None, None),
        P(None, "tm"),
        P(None, "tm"),
        P(None, "tm"),
        P("tm", None),
        P(None, "tm"),
        P(),
        P(),
        P("tm", None, None),
        P(None, "tm"),
        P(None, "tm"),
        P(None, "tm"),
        P("tm", None),
        P(None, "tm"),
        P(),
    )
    out_specs = (P("batch", None, "tm"), P())
    return jax.shard_map(
        per_device, mesh=mesh, in_specs=in_specs, out_specs=out_specs, check_vma=False
    )
```

```python
import functools
import math

import jax
import jax.numpy as jnp
from jax import lax
from jax.experimental import pallas as pl
from jax.experimental.pallas import tpu as pltpu
from jax.sharding import PartitionSpec as P

HD = 128
FREQ = 256
FTOK = 128


norm_floor = 0.05
gap_floor = 0.25
highest = lax.Precision.HIGHEST


MESH = pl.DeviceIdType.MESH
f32 = jnp.float32
bf16 = jnp.bfloat16


def greet(sizes):
    barrier = pltpu.get_barrier_semaphore()
    count = 0
    for axis, size in sizes.items():
        me = lax.axis_index(axis)
        for k in range(1, size):
            pl.semaphore_signal(
                barrier, inc=1, device_id={axis: lax.rem(me + k, size)}, device_id_type=MESH
            )
            count += 1
    pl.semaphore_wait(barrier, count)


def exchange(axis, size, source, slots, send, recv):
    me = lax.axis_index(axis)
    copies = []
    for k in range(1, size):
        peer = lax.rem(me + k, size)
        copy = pltpu.make_async_remote_copy(
            src_ref=source(peer),
            dst_ref=slots.at[me],
            send_sem=send.at[k],
            recv_sem=recv.at[k],
            device_id={axis: peer},
            device_id_type=MESH,
        )
        copy.start()
        copies.append(copy)
    return copies


def landed(copies):
    for copy in copies:
        copy.wait_recv()


def gone(copies):
    for copy in copies:
        copy.wait_send()


def sems(*sizes):
    return [pltpu.SemaphoreType.DMA((size,)) for size in sizes for _ in range(2)]


def split(wide):
    high = wide.astype(bf16)
    return high, (wide - high.astype(f32)).astype(bf16)


def dot_nt(left, right):
    return lax.dot_general(left, right, (((1,), (1,)), ((), ())), preferred_element_type=f32)


def dot(left, right):
    return jnp.dot(left, right, preferred_element_type=f32)


def main_kernel(n, nb, part, level_ref, noisy_ref, made_ref, share_ref, gain_ref, *refs):
    big, refs = refs[:13], refs[13:]
    (dmd_ref, weight_ref), refs = refs[:2], refs[2:]
    held, refs = refs[:13], refs[13:]
    (load_sem, patches, parts, modul, fold, gate_fold, gram, inner, stack, qkv, squares,
     square_parts, keys, terms, term_parts, gap, gaps, halves, partner, across_chips, reduced,
     chip_parts, mixed, quarters, merged, grad) = refs[:26]
    sem = refs[26:]
    me = lax.axis_index("tm")
    mine = lax.axis_index("batch")
    core, chip = lax.rem(me, 2), lax.div(me, 2)
    chips = n // 2
    patch_rows, frame = noisy_ref.shape
    tokens = n * frame
    width = held[0].shape[1]
    chunks = width // part
    loads = []
    for i, (source, target) in enumerate(zip(big, held)):
        load = pltpu.make_async_copy(source, target, load_sem.at[i])
        load.start()
        loads.append(load)
    nets = [held[6 * i : 6 * i + 6] for i in (0, 1)]
    hidden = held[12]

    greet({"tm": n, "batch": nb})
    scatter = exchange("tm", n, lambda peer: share_ref.at[peer], parts, sem[0], sem[1])
    spread = exchange("tm", n, lambda peer: noisy_ref, patches, sem[2], sem[3])
    parts[me] = share_ref[me]
    patches[me] = noisy_ref[...]
    landed(scatter)
    modul[me] = jnp.sum(parts[...], axis=0)
    collect = exchange("tm", n, lambda peer: modul.at[me], modul, sem[4], sem[5])

    def columns(s):
        return pl.ds(pl.multiple_of(s * part, 128), part)

    means = []
    for i, (embed, proj, query, key, value, out) in enumerate(nets):
        loads[6 * i].wait()
        loads[6 * i + 1].wait()
        mean = jnp.sum(embed[...].astype(f32), axis=1, keepdims=True) / width
        means.append(mean)
        gram[i] = jnp.zeros(gram.shape[1:], f32)
        inner[i] = jnp.zeros(inner.shape[1:], f32)

        def gram_step(s, carry):
            table = embed[:, columns(s)]
            high, low = split(table.astype(f32) - mean)
            own = dot_nt(high, high)
            cross = dot_nt(high, low)
            gram[i] += own + cross + cross.T
            inner[i] += dot_nt(proj[:, columns(s)], table)
            return carry

        lax.fori_loop(0, chunks, gram_step, 0)

    landed(spread)
    kin = 2 * patch_rows
    for s in range(n):
        at = slice(s * frame, (s + 1) * frame)
        now = patches[s]
        before = patches[s - 1] if s else jnp.zeros_like(now)
        both = jnp.concatenate([now, before], axis=0)
        stack[:kin, at] = both
        stack[kin:, at] = both
    landed(collect)

    head = qkv.shape[1] // 3
    for i, (embed, proj, query, key, value, out) in enumerate(nets):
        for j in range(2, 6):
            loads[6 * i + j].wait()
        mean = means[i]
        fold[...] = jnp.zeros_like(fold)
        gate_fold[i] = jnp.zeros(gate_fold.shape[1:], f32)

        def fold_step(s, carry):
            at = columns(s)
            rows = modul[s]
            shift, scale, gate = (rows[3 * i + j : 3 * i + j + 1] for j in range(3))
            high, low = split((embed[:, at].astype(f32) - mean) * (1.0 + scale))
            shift_high, shift_low = split(jnp.broadcast_to(shift, (16, part)))
            left = jnp.concatenate([high, low, shift_high, shift_low], axis=0)
            right = jnp.concatenate([query[at, :], key[at, :], value[at, :]], axis=1)
            fold[...] += dot(left, right)
            high, low = split(proj[:, at].astype(f32) * gate)
            gate_fold[i] += dot_nt(jnp.concatenate([high, low], axis=0), out[:, at])
            return carry

        lax.fori_loop(0, chunks, fold_step, 0)
        folded = (fold[:kin] + fold[kin : 2 * kin]).T
        offset = (fold[2 * kin : 2 * kin + 8] + fold[2 * kin + 16 : 2 * kin + 24]).T[:, :1]
        gram_pair = jnp.concatenate(split(gram[i] / width), axis=1)
        fold_pair = jnp.concatenate(split(folded), axis=1)

        for s in range(n):
            at = slice(s * frame, (s + 1) * frame)
            pair = stack[:, at]
            variance = jnp.sum(pair[:kin].astype(f32) * dot(gram_pair, pair), axis=0, keepdims=True)
            rscale = lax.rsqrt(jnp.maximum(variance, 0.0) + norm_floor)
            full = dot(fold_pair, pair) * rscale + offset
            qkv[i, :, at] = full
            for j in range(2):
                rows = full[j * head : (j + 1) * head]
                squares[2 * i + j : 2 * i + j + 1, at] = jnp.sum(rows * rows, axis=0, keepdims=True)

    sums = exchange("tm", n, lambda peer: squares, square_parts, sem[6], sem[7])
    square_parts[me] = squares[...]
    landed(sums)
    inverse = lax.rsqrt(jnp.sum(square_parts[...], axis=0) / (head * n) + norm_floor)

    block = 2 * frame
    groups = min(4, tokens // block)
    per_group = tokens // block // groups
    for i in range(2):
        for s in range(n):
            at = slice(s * frame, (s + 1) * frame)
            gained = qkv[i, head : 2 * head, at] * inverse[2 * i + 1 : 2 * i + 2, at]
            keys[i, at, :] = (gained * gain_ref[i, :, 1:2]).T.astype(bf16)
            gained = qkv[i, :head, at] * inverse[2 * i : 2 * i + 1, at]
            qkv[i, :head, at] = gained * gain_ref[i, :, 0:1]
    fold_outs = [
        (gate_fold[i, :patch_rows] + gate_fold[i, patch_rows:]).astype(bf16) for i in range(2)
    ]
    for group in range(groups):
        length = (group + 1) * per_group * block

        def block_step(b, carry):
            at = pl.ds(pl.multiple_of(b * block, block), block)
            for i in range(2):
                query = qkv[i, :head, at].astype(bf16)
                scores = dot(keys[i, :length], query)
                low = (length - per_group * block)
                key_frame = (lax.broadcasted_iota(jnp.int32, (length - low, block), 0) + low) // frame
                query_frame = (
                    lax.broadcasted_iota(jnp.int32, (length - low, block), 1) + b * block
                ) // frame
                edge = jnp.where(key_frame <= query_frame, scores[low:], -1e30)
                if low:
                    scores = jnp.concatenate([scores[:low], edge], axis=0)
                else:
                    scores = edge
                peak = jnp.max(scores, axis=0, keepdims=True)
                powers = jnp.exp((scores - peak) * (1.0 / math.sqrt(HD)))
                total = jnp.sum(powers, axis=0, keepdims=True)
                values = qkv[i, 2 * head :, :length].astype(bf16)
                attended = dot(values, powers.astype(bf16)) / total
                term = dot(fold_outs[i], attended.astype(bf16)).astype(bf16)
                for j in range(2):
                    terms[2 * b + j, i * patch_rows : (i + 1) * patch_rows] = term[
                        :, j * frame : (j + 1) * frame
                    ]
            return carry

        if per_group == 1:
            block_step(group, 0)
        else:
            lax.fori_loop(group * per_group, (group + 1) * per_group, block_step, 0)

    give = exchange("tm", n, lambda peer: terms.at[peer], term_parts, sem[8], sem[9])
    term_parts[me] = terms[me]
    own = stack[:, pl.ds(pl.multiple_of(me * frame, frame), frame)]
    direct = [dot(jnp.concatenate(split(inner[i]), axis=1), own) for i in range(2)]
    noisy = noisy_ref[...].astype(f32)
    level = level_ref[:1, :1]
    landed(give)
    summed = jnp.sum(term_parts[...].astype(f32), axis=0)
    pred_real = noisy - level * (summed[:patch_rows] + direct[0])
    pred_fake = noisy - level * (summed[patch_rows:] + direct[1])
    difference = pred_fake - pred_real
    distance = jnp.abs(made_ref[...].astype(f32) - pred_real)
    distance = jnp.sum(jnp.sum(distance, axis=0, keepdims=True), axis=1, keepdims=True)
    gap[...] = jnp.broadcast_to(distance, gap.shape)
    gap_copies = exchange("tm", n, lambda peer: gap, gaps, sem[10], sem[11])
    gaps[me] = gap[...]
    loads[12].wait()
    rounded = difference.astype(bf16)
    for s in range(n):
        if s < chunks:
            piece = dot(rounded, hidden[:, s * part : (s + 1) * part]).astype(bf16)
        else:
            piece = jnp.zeros(halves.shape[2:], bf16)
        halves[s % 2, s // 2] = piece
    swap = pltpu.make_async_remote_copy(
        src_ref=halves.at[1 - core],
        dst_ref=partner,
        send_sem=sem[12].at[0],
        recv_sem=sem[12].at[1],
        device_id={"tm": me + 1 - 2 * core},
        device_id_type=MESH,
    )
    swap.start()
    swap.wait_recv()
    for k in range(chips):
        reduced[k] = (halves[core, k].astype(f32) + partner[k].astype(f32)).astype(bf16)

    def between_chips(source, slots, send, recv):
        copies = []
        for k in range(1, chips):
            peer = lax.rem(chip + k, chips)
            copy = pltpu.make_async_remote_copy(
                src_ref=source(peer),
                dst_ref=slots(chip),
                send_sem=send.at[k],
                recv_sem=recv.at[k],
                device_id={"tm": 2 * peer + core},
                device_id_type=MESH,
            )
            copy.start()
            copies.append(copy)
        return copies

    chip_copies = between_chips(
        lambda peer: reduced.at[peer], lambda at: chip_parts.at[at], sem[13], sem[14]
    )
    chip_parts[chip] = reduced[chip]
    landed(gap_copies)
    normalizer = jnp.maximum(jnp.sum(gaps[...], axis=0) / (patch_rows * tokens), gap_floor)[:1, :1]
    dmd_ref[...] = difference / normalizer
    landed(chip_copies)
    grad_root = math.sqrt(nb * tokens)
    total = jnp.sum(chip_parts[...].astype(f32), axis=0) / normalizer / grad_root
    mixed[...] = total.reshape(mixed.shape).astype(bf16)
    across = exchange("batch", nb, lambda peer: mixed.at[peer], quarters, sem[15], sem[16])
    quarters[mine] = mixed[mine]
    landed(across)
    merged[mine] = jnp.sum(quarters[...].astype(f32), axis=0).astype(bf16)
    back = exchange("batch", nb, lambda peer: merged.at[mine], merged, sem[17], sem[18])
    landed(back)
    grad[core, chip] = merged[...]
    last = between_chips(lambda peer: merged, lambda at: grad.at[core, at], sem[19], sem[20])
    landed(last)
    share = pltpu.make_async_remote_copy(
        src_ref=grad.at[core],
        dst_ref=grad.at[core],
        send_sem=sem[12].at[2],
        recv_sem=sem[12].at[3],
        device_id={"tm": me + 1 - 2 * core},
        device_id_type=MESH,
    )
    share.start()
    share.wait_recv()
    for s in range(chunks):
        piece = grad[s % 2, s // 2].astype(f32)
        weight_ref[:, s * part : (s + 1) * part] = piece.reshape(patch_rows, part)
    swap.wait_send()
    share.wait_send()
    for copies in (
        scatter, spread, collect, sums, give, gap_copies, chip_copies, across, back, last
    ):
        gone(copies)


def sinusoid(time_step):
    half_freq = FREQ // 2
    frequency = jnp.exp(-math.log(10000.0) * jnp.arange(half_freq, dtype=jnp.float32) / half_freq)
    angles = time_step.astype(jnp.float32) * frequency
    return jnp.concatenate([jnp.cos(angles), jnp.sin(angles)]).astype(jnp.bfloat16)


def per_device(
    hidden_states,
    gen_weight,
    noise_field,
    timesteps,
    embed_real,
    time_real,
    query_real,
    key_real,
    value_real,
    out_real,
    gain_real,
    proj_real,
    embed_fake,
    time_fake,
    query_fake,
    key_fake,
    value_fake,
    out_fake,
    gain_fake,
    proj_fake,
):
    devices = lax.axis_size("tm")
    frame_tokens = hidden_states.shape[1]
    tokens = frame_tokens * devices
    patch_rows = gen_weight.shape[0]
    time_step = timesteps[0]
    level_raw = time_step.astype(jnp.float32) / 1000.0
    noise_level = 5.0 * level_raw / (1.0 + 4.0 * level_raw)
    generated = lax.dot_general(
        gen_weight, hidden_states[0], (((1,), (1,)), ((), ())), preferred_element_type=f32
    ).astype(bf16)
    noisy_patch = (
        (1.0 - noise_level) * generated.astype(f32) + noise_level * noise_field[0].astype(f32)
    ).astype(bf16)
    sinus_wave = sinusoid(time_step)
    freq_rows = time_real.shape[0]
    own_wave = lax.dynamic_slice_in_dim(sinus_wave, lax.axis_index("tm") * freq_rows, freq_rows, 0)
    model_width = hidden_states.shape[2]
    batches = lax.axis_size("batch")
    part = -(-model_width // (devices * 128)) * 128
    while model_width % part:
        part += 128
    padding = ((0, 0), (0, devices * part - model_width))
    shares = jnp.concatenate(
        [
            jnp.dot(own_wave[None], t.reshape(freq_rows, -1), preferred_element_type=f32).reshape(
                3, model_width
            )
            for t in (time_real, time_fake)
        ]
    )
    shares = jnp.pad(shares, padding).reshape(6, devices, part).transpose(1, 0, 2)
    n, chips, quarter, head = devices, devices // 2, patch_rows // batches, query_real.shape[1]
    kin = 2 * patch_rows
    big = (
        embed_real, proj_real, query_real, key_real, value_real, out_real,
        embed_fake, proj_fake, query_fake, key_fake, value_fake, out_fake,
        hidden_states[0],
    )
    vm = pltpu.VMEM
    scratch = [
        *[vm(array.shape, array.dtype) for array in big],
        pltpu.SemaphoreType.DMA((len(big),)),
        vm((n, patch_rows, frame_tokens), bf16),
        vm((n, 6, part), f32),
        vm((n, 6, part), f32),
        vm((2 * kin + 32, 3 * head), f32),
        vm((2, kin, head), f32),
        vm((2, kin, kin), f32),
        vm((2, patch_rows, kin), f32),
        vm((2 * kin, tokens), bf16),
        vm((2, 3 * head, tokens), f32),
        vm((4, tokens), f32),
        vm((n, 4, tokens), f32),
        vm((2, tokens, head), bf16),
        vm((n, kin, frame_tokens), bf16),
        vm((n, kin, frame_tokens), bf16),
        vm((8, 128), f32),
        vm((n, 8, 128), f32),
        vm((2, chips, patch_rows, part), bf16),
        vm((chips, patch_rows, part), bf16),
        vm((8, 128), f32),
        vm((chips, patch_rows, part), bf16),
        vm((chips, patch_rows, part), bf16),
        vm((batches, quarter, part), bf16),
        vm((batches, quarter, part), bf16),
        vm((batches, quarter, part), bf16),
        vm((2, chips, batches, quarter, part), bf16),
        *sems(n, n, n, n, n, n),
        pltpu.SemaphoreType.DMA((4,)),
        *sems(chips, batches, batches, chips),
    ]
    vmem = pl.BlockSpec(memory_space=pltpu.VMEM)
    dmd, weight_grad = pl.pallas_call(
        functools.partial(main_kernel, devices, batches, part),
        out_shape=[
            jax.ShapeDtypeStruct((patch_rows, frame_tokens), f32),
            jax.ShapeDtypeStruct((patch_rows, model_width), f32),
        ],
        in_specs=[vmem] * 5 + [pl.BlockSpec(memory_space=pl.ANY)] * len(big),
        out_specs=[vmem, vmem],
        scratch_shapes=scratch,
        compiler_params=pltpu.CompilerParams(
            collective_id=0, has_side_effects=True, vmem_limit_bytes=60 * 1024 * 1024
        ),
    )(
        jnp.broadcast_to(noise_level, (8, 128)),
        noisy_patch,
        generated,
        shares,
        jnp.stack([gain_real.T, gain_fake.T]),
        *big,
    )
    return (dmd[None], weight_grad)


def solution(mesh):
    in_specs = (
        P("batch", "tm", None),
        P(),
        P("batch", None, "tm"),
        P("batch"),
        P(),
        P("tm", None, None),
        P(None, "tm"),
        P(None, "tm"),
        P(None, "tm"),
        P("tm", None),
        P(None, "tm"),
        P(),
        P(),
        P("tm", None, None),
        P(None, "tm"),
        P(None, "tm"),
        P(None, "tm"),
        P("tm", None),
        P(None, "tm"),
        P(),
    )
    out_specs = (P("batch", None, "tm"), P())
    return jax.shard_map(
        per_device, mesh=mesh, in_specs=in_specs, out_specs=out_specs, check_vma=False
    )
```

```python
import functools
import math

import jax
import jax.numpy as jnp
from jax import lax
from jax.experimental import pallas as pl
from jax.experimental.pallas import tpu as pltpu
from jax.sharding import PartitionSpec as P

HD = 128
FREQ = 256
FTOK = 128


norm_floor = 0.05
gap_floor = 0.25
highest = lax.Precision.HIGHEST


MESH = pl.DeviceIdType.MESH
f32 = jnp.float32
bf16 = jnp.bfloat16


def hail(sizes):
    barrier = pltpu.get_barrier_semaphore()
    for axis, size in sizes.items():
        me = lax.axis_index(axis)
        for k in range(1, size):
            pl.semaphore_signal(
                barrier, inc=1, device_id={axis: lax.rem(me + k, size)}, device_id_type=MESH
            )


def meet(sizes):
    count = sum(size - 1 for size in sizes.values())
    pl.semaphore_wait(pltpu.get_barrier_semaphore(), count)


def exchange(axis, size, source, slots, send, recv):
    me = lax.axis_index(axis)
    copies = []
    for k in range(1, size):
        peer = lax.rem(me + k, size)
        copy = pltpu.make_async_remote_copy(
            src_ref=source(peer),
            dst_ref=slots.at[me],
            send_sem=send.at[k],
            recv_sem=recv.at[k],
            device_id={axis: peer},
            device_id_type=MESH,
        )
        copy.start()
        copies.append(copy)
    return copies


def landed(copies):
    for copy in copies:
        copy.wait_recv()


def gone(copies):
    for copy in copies:
        copy.wait_send()


def sems(*sizes):
    return [pltpu.SemaphoreType.DMA((size,)) for size in sizes for _ in range(2)]


def split(wide):
    high = wide.astype(bf16)
    return high, (wide - high.astype(f32)).astype(bf16)


def dot_nt(left, right):
    return lax.dot_general(left, right, (((1,), (1,)), ((), ())), preferred_element_type=f32)


def dot(left, right):
    return jnp.dot(left, right, preferred_element_type=f32)


def main_kernel(n, nb, part, level_ref, wave_ref, noise_ref, gain_real, gain_fake, *refs):
    big, refs = refs[:16], refs[16:]
    (difference_ref, norm_ref, weight_ref), refs = refs[:3], refs[3:]
    held, refs = refs[:16], refs[16:]
    (load_sem, patches, parts, modul, fold, gate_fold, gram, inner, stack, qkv, squares,
     square_parts, keys, terms, term_parts, gap, gaps, noisy_ref, share_ref, columns_held, rounded,
     all_rounded, mixed, quarters, merged, grad) = refs[:26]
    sem = refs[26:]
    me = lax.axis_index("tm")
    mine = lax.axis_index("batch")
    core, chip = lax.rem(me, 2), lax.div(me, 2)
    chips = n // 2
    patch_rows, frame = noisy_ref.shape
    level = level_ref[0, 0]
    tokens = n * frame
    width = held[0].shape[1]
    chunks = width // part
    loads = []
    for i, (source, target) in enumerate(zip(big, held)):
        loads.append(pltpu.make_async_copy(source, target, load_sem.at[i]))
    for i in (13, 12, 14, 15, *range(12)):
        loads[i].start()
    nets = [held[6 * i : 6 * i + 6] for i in (0, 1)]
    hidden = held[12]

    hail({"tm": n, "batch": nb})
    loads[13].wait()
    loads[12].wait()
    made = dot_nt(held[13][...], hidden[...]).astype(bf16).astype(f32)
    noisy = ((1.0 - level) * made + level * noise_ref[...].astype(f32)).astype(bf16)
    noisy_ref[...] = noisy
    noisy = noisy.astype(f32)
    for i in (0, 1):
        loads[14 + i].wait()
        for j in range(3):
            share = dot(wave_ref[...], held[14 + i][j])
            for s in range(n):
                if s < chunks:
                    row = share[:1, s * part : (s + 1) * part]
                else:
                    row = jnp.zeros((1, part), f32)
                share_ref[s, 3 * i + j : 3 * i + j + 1] = row
    meet({"tm": n, "batch": nb})
    scatter = exchange("tm", n, lambda peer: share_ref.at[peer], parts, sem[0], sem[1])
    spread = exchange("tm", n, lambda peer: noisy_ref, patches, sem[2], sem[3])
    parts[me] = share_ref[me]
    patches[me] = noisy_ref[...]
    landed(scatter)
    modul[me] = jnp.sum(parts[...], axis=0)
    collect = exchange("tm", n, lambda peer: modul.at[me], modul, sem[4], sem[5])

    def columns(s):
        return pl.ds(pl.multiple_of(s * part, 128), part)

    def own_columns(peer):
        return hidden.at[:, columns(lax.rem(peer, chunks))]

    pass_hidden = exchange("tm", n, own_columns, columns_held, sem[10], sem[11])
    columns_held[me] = hidden[:, columns(lax.rem(me, chunks))]

    means = []
    for i, (embed, proj, query, key, value, out) in enumerate(nets):
        loads[6 * i].wait()
        loads[6 * i + 1].wait()
        mean = jnp.sum(embed[...].astype(f32), axis=1, keepdims=True) / width
        means.append(mean)
        gram[i] = jnp.zeros(gram.shape[1:], f32)
        inner[i] = jnp.zeros(inner.shape[1:], f32)

        def gram_step(s, carry):
            table = embed[:, columns(s)]
            high, low = split(table.astype(f32) - mean)
            own = dot_nt(high, high)
            cross = dot_nt(high, low)
            gram[i] += own + cross + cross.T
            inner[i] += dot_nt(proj[:, columns(s)], table)
            return carry

        lax.fori_loop(0, chunks, gram_step, 0)

    landed(spread)
    kin = 2 * patch_rows
    for s in range(n):
        at = slice(s * frame, (s + 1) * frame)
        now = patches[s]
        before = patches[s - 1] if s else jnp.zeros_like(now)
        both = jnp.concatenate([now, before], axis=0)
        stack[:kin, at] = both
        stack[kin:, at] = both
    landed(collect)

    head = qkv.shape[1] // 3
    for i, (embed, proj, query, key, value, out) in enumerate(nets):
        for j in range(2, 6):
            loads[6 * i + j].wait()
        mean = means[i]
        fold[...] = jnp.zeros_like(fold)
        gate_fold[i] = jnp.zeros(gate_fold.shape[1:], f32)

        def fold_step(s, carry):
            at = columns(s)
            rows = modul[s]
            shift, scale, gate = (rows[3 * i + j : 3 * i + j + 1] for j in range(3))
            high, low = split((embed[:, at].astype(f32) - mean) * (1.0 + scale))
            shift_high, shift_low = split(jnp.broadcast_to(shift, (16, part)))
            left = jnp.concatenate([high, low, shift_high, shift_low], axis=0)
            right = jnp.concatenate([query[at, :], key[at, :], value[at, :]], axis=1)
            fold[...] += dot(left, right)
            high, low = split(proj[:, at].astype(f32) * gate)
            gate_fold[i] += dot_nt(jnp.concatenate([high, low], axis=0), out[:, at])
            return carry

        lax.fori_loop(0, chunks, fold_step, 0)
        folded = (fold[:kin] + fold[kin : 2 * kin]).T
        offset = (fold[2 * kin : 2 * kin + 8] + fold[2 * kin + 16 : 2 * kin + 24]).T[:, :1]
        gram_pair = jnp.concatenate(split(gram[i] / width), axis=1)
        fold_pair = jnp.concatenate(split(folded), axis=1)

        for s in range(n):
            at = slice(s * frame, (s + 1) * frame)
            pair = stack[:, at]
            variance = jnp.sum(pair[:kin].astype(f32) * dot(gram_pair, pair), axis=0, keepdims=True)
            rscale = lax.rsqrt(jnp.maximum(variance, 0.0) + norm_floor)
            full = dot(fold_pair, pair) * rscale + offset
            qkv[i, :, at] = full
            for j in range(2):
                rows = full[j * head : (j + 1) * head]
                squares[2 * i + j : 2 * i + j + 1, at] = jnp.sum(rows * rows, axis=0, keepdims=True)

    sums = exchange("tm", n, lambda peer: squares, square_parts, sem[6], sem[7])
    square_parts[me] = squares[...]
    landed(sums)
    inverse = lax.rsqrt(jnp.sum(square_parts[...], axis=0) / (head * n) + norm_floor)

    block = 2 * frame
    groups = min(4, tokens // block)
    gains = [ref[0:1, :] * ref[1:2, :] for ref in (gain_real, gain_fake)]
    per_group = tokens // block // groups
    for i in range(2):
        for s in range(n):
            at = slice(s * frame, (s + 1) * frame)
            gained = qkv[i, head : 2 * head, at] * inverse[2 * i + 1 : 2 * i + 2, at]
            keys[i, at, :] = (gained.T * gains[i]).astype(bf16)
            qkv[i, :head, at] = qkv[i, :head, at] * inverse[2 * i : 2 * i + 1, at]
    fold_outs = [
        (gate_fold[i, :patch_rows] + gate_fold[i, patch_rows:]).astype(bf16) for i in range(2)
    ]
    for group in range(groups):
        length = (group + 1) * per_group * block

        def block_step(b, carry):
            at = pl.ds(pl.multiple_of(b * block, block), block)
            for i in range(2):
                query = qkv[i, :head, at].astype(bf16)
                scores = dot(keys[i, :length], query)
                low = (length - per_group * block)
                key_frame = (lax.broadcasted_iota(jnp.int32, (length - low, block), 0) + low) // frame
                query_frame = (
                    lax.broadcasted_iota(jnp.int32, (length - low, block), 1) + b * block
                ) // frame
                edge = jnp.where(key_frame <= query_frame, scores[low:], -1e30)
                if low:
                    scores = jnp.concatenate([scores[:low], edge], axis=0)
                else:
                    scores = edge
                peak = jnp.max(scores, axis=0, keepdims=True)
                powers = jnp.exp((scores - peak) * (1.0 / math.sqrt(HD)))
                total = jnp.sum(powers, axis=0, keepdims=True)
                values = qkv[i, 2 * head :, :length].astype(bf16)
                attended = dot(values, powers.astype(bf16)) / total
                term = dot(fold_outs[i], attended.astype(bf16)).astype(bf16)
                for j in range(2):
                    terms[2 * b + j, i * patch_rows : (i + 1) * patch_rows] = term[
                        :, j * frame : (j + 1) * frame
                    ]
            return carry

        if per_group == 1:
            block_step(group, 0)
        else:
            lax.fori_loop(group * per_group, (group + 1) * per_group, block_step, 0)

    give = exchange("tm", n, lambda peer: terms.at[peer], term_parts, sem[8], sem[9])
    term_parts[me] = terms[me]
    own = stack[:, pl.ds(pl.multiple_of(me * frame, frame), frame)]
    direct = [dot(jnp.concatenate(split(inner[i]), axis=1), own) for i in range(2)]
    landed(give)
    summed = jnp.sum(term_parts[...].astype(f32), axis=0)
    pred_real = noisy - level * (summed[:patch_rows] + direct[0])
    pred_fake = noisy - level * (summed[patch_rows:] + direct[1])
    difference = pred_fake - pred_real
    distance = jnp.abs(made - pred_real)
    distance = jnp.sum(jnp.sum(distance, axis=0, keepdims=True), axis=1, keepdims=True)
    gap[...] = jnp.broadcast_to(distance, gap.shape)
    rounded[...] = difference.astype(bf16)
    difference_copies = exchange("tm", n, lambda peer: rounded, all_rounded, sem[12], sem[13])
    gap_copies = exchange("tm", n, lambda peer: gap, gaps, sem[14], sem[15])
    gaps[me] = gap[...]
    all_rounded[me] = rounded[...]
    difference_ref[...] = difference
    landed(pass_hidden)
    landed(difference_copies)
    total = dot(all_rounded[0], columns_held[0])
    for s in range(1, n):
        total = total + dot(all_rounded[s], columns_held[s])
    landed(gap_copies)
    normalizer = jnp.maximum(jnp.sum(gaps[...], axis=0) / (patch_rows * tokens), gap_floor)
    norm_ref[...] = normalizer
    total = total / normalizer[:1, :1] / math.sqrt(nb * tokens)
    mixed[...] = total.reshape(mixed.shape).astype(bf16)
    across = exchange("batch", nb, lambda peer: mixed.at[peer], quarters, sem[16], sem[17])
    quarters[mine] = mixed[mine]
    landed(across)
    merged[mine] = jnp.sum(quarters[...].astype(f32), axis=0).astype(bf16)
    back = exchange("batch", nb, lambda peer: merged.at[mine], merged, sem[18], sem[19])

    grad[core, chip, mine] = merged[mine]
    chain = []

    def to_chips(piece, k):
        copies = []
        for hop in range(1, chips):
            peer = lax.rem(chip + hop, chips)
            copy = pltpu.make_async_remote_copy(
                src_ref=merged.at[piece],
                dst_ref=grad.at[core, chip, piece],
                send_sem=sem[20].at[k * chips + hop],
                recv_sem=sem[21].at[k * chips + hop],
                device_id={"tm": 2 * peer + core},
                device_id_type=MESH,
            )
            copy.start()
            copies.append(copy)
        return copies

    chain.append(to_chips(mine, 0))
    for k in range(1, nb):
        back[k - 1].wait_recv()
        piece = lax.rem(mine + nb - k, nb)
        grad[core, chip, piece] = merged[piece]
        chain.append(to_chips(piece, k))

    def to_partner(at, hop):
        copy = pltpu.make_async_remote_copy(
            src_ref=grad.at[core, at],
            dst_ref=grad.at[core, at],
            send_sem=sem[22].at[hop],
            recv_sem=sem[23].at[hop],
            device_id={"tm": me + 1 - 2 * core},
            device_id_type=MESH,
        )
        copy.start()
        return copy

    shares = [to_partner(chip, 0)]
    for hop in range(1, chips):
        for copies in chain:
            copies[hop - 1].wait_recv()
        shares.append(to_partner(lax.rem(chip + chips - hop, chips), hop))
    landed(shares)
    for s in range(chunks):
        piece = grad[s % 2, s // 2]
        weight_ref[:, s * part : (s + 1) * part] = piece.reshape(patch_rows, part)
    for copies in (
        scatter, spread, collect, pass_hidden, sums, give, difference_copies, gap_copies,
        across, back, *chain, shares,
    ):
        gone(copies)


def sinusoid(time_step):
    half_freq = FREQ // 2
    frequency = jnp.exp(-math.log(10000.0) * jnp.arange(half_freq, dtype=jnp.float32) / half_freq)
    angles = time_step.astype(jnp.float32) * frequency
    return jnp.concatenate([jnp.cos(angles), jnp.sin(angles)]).astype(jnp.bfloat16)


def per_device(
    hidden_states,
    gen_weight,
    noise_field,
    timesteps,
    embed_real,
    time_real,
    query_real,
    key_real,
    value_real,
    out_real,
    gain_real,
    proj_real,
    embed_fake,
    time_fake,
    query_fake,
    key_fake,
    value_fake,
    out_fake,
    gain_fake,
    proj_fake,
):
    devices = lax.axis_size("tm")
    frame_tokens = hidden_states.shape[1]
    tokens = frame_tokens * devices
    patch_rows = gen_weight.shape[0]
    time_step = timesteps[0]
    level_raw = time_step.astype(jnp.float32) / 1000.0
    noise_level = 5.0 * level_raw / (1.0 + 4.0 * level_raw)
    sinus_wave = sinusoid(time_step)
    freq_rows = time_real.shape[0]
    own_wave = lax.dynamic_slice_in_dim(sinus_wave, lax.axis_index("tm") * freq_rows, freq_rows, 0)
    model_width = hidden_states.shape[2]
    batches = lax.axis_size("batch")
    part = -(-model_width // (devices * 128)) * 128
    while model_width % part:
        part += 128
    n, chips, quarter, head = devices, devices // 2, patch_rows // batches, query_real.shape[1]
    kin = 2 * patch_rows
    big = (
        embed_real, proj_real, query_real, key_real, value_real, out_real,
        embed_fake, proj_fake, query_fake, key_fake, value_fake, out_fake,
        hidden_states[0], gen_weight,
        time_real.transpose(1, 0, 2), time_fake.transpose(1, 0, 2),
    )
    vm = pltpu.VMEM
    scratch = [
        *[vm(array.shape, array.dtype) for array in big],
        pltpu.SemaphoreType.DMA((len(big),)),
        vm((n, patch_rows, frame_tokens), bf16),
        vm((n, 6, part), f32),
        vm((n, 6, part), f32),
        vm((2 * kin + 32, 3 * head), f32),
        vm((2, kin, head), f32),
        vm((2, kin, kin), f32),
        vm((2, patch_rows, kin), f32),
        vm((2 * kin, tokens), bf16),
        vm((2, 3 * head, tokens), f32),
        vm((4, tokens), f32),
        vm((n, 4, tokens), f32),
        vm((2, tokens, head), bf16),
        vm((n, kin, frame_tokens), bf16),
        vm((n, kin, frame_tokens), bf16),
        vm((8, 128), f32),
        vm((n, 8, 128), f32),
        vm((patch_rows, frame_tokens), bf16),
        vm((n, 6, part), f32),
        vm((n, frame_tokens, part), bf16),
        vm((patch_rows, frame_tokens), bf16),
        vm((n, patch_rows, frame_tokens), bf16),
        vm((batches, quarter, part), bf16),
        vm((batches, quarter, part), bf16),
        vm((batches, quarter, part), bf16),
        vm((2, chips, batches, quarter, part), bf16),
        *sems(n, n, n, n, n, n, n, n, batches, batches, batches * chips, chips),
    ]
    vmem = pl.BlockSpec(memory_space=pltpu.VMEM)
    difference, norm, weight_grad = pl.pallas_call(
        functools.partial(main_kernel, devices, batches, part),
        out_shape=[
            jax.ShapeDtypeStruct((patch_rows, frame_tokens), f32),
            jax.ShapeDtypeStruct((8, 128), f32),
            jax.ShapeDtypeStruct((patch_rows, model_width), bf16),
        ],
        in_specs=[pl.BlockSpec(memory_space=pltpu.SMEM)] + [vmem] * 4 + [pl.BlockSpec(memory_space=pl.ANY)] * len(big),
        out_specs=[vmem] * 3,
        scratch_shapes=scratch,
        compiler_params=pltpu.CompilerParams(
            collective_id=0, has_side_effects=True, vmem_limit_bytes=60 * 1024 * 1024
        ),
    )(
        noise_level.reshape(1, 1),
        jnp.broadcast_to(own_wave, (16, freq_rows)),
        noise_field[0],
        gain_real,
        gain_fake,
        *big,
    )
    return ((difference / norm[0, 0])[None], weight_grad.astype(f32))


def solution(mesh):
    in_specs = (
        P("batch", "tm", None),
        P(),
        P("batch", None, "tm"),
        P("batch"),
        P(),
        P("tm", None, None),
        P(None, "tm"),
        P(None, "tm"),
        P(None, "tm"),
        P("tm", None),
        P(None, "tm"),
        P(),
        P(),
        P("tm", None, None),
        P(None, "tm"),
        P(None, "tm"),
        P(None, "tm"),
        P("tm", None),
        P(None, "tm"),
        P(),
    )
    out_specs = (P("batch", None, "tm"), P())
    return jax.shard_map(
        per_device, mesh=mesh, in_specs=in_specs, out_specs=out_specs, check_vma=False
    )
```

```python
import functools
import math

import jax
import jax.numpy as jnp
from jax import lax
from jax.experimental import pallas as pl
from jax.experimental.pallas import tpu as pltpu
from jax.sharding import PartitionSpec as P

HD = 128
FREQ = 256
FTOK = 128


norm_floor = 0.05
gap_floor = 0.25
highest = lax.Precision.HIGHEST


MESH = pl.DeviceIdType.MESH
f32 = jnp.float32
bf16 = jnp.bfloat16


def hail(sizes):
    barrier = pltpu.get_barrier_semaphore()
    for axis, size in sizes.items():
        me = lax.axis_index(axis)
        for k in range(1, size):
            pl.semaphore_signal(
                barrier, inc=1, device_id={axis: lax.rem(me + k, size)}, device_id_type=MESH
            )


def meet(sizes):
    count = sum(size - 1 for size in sizes.values())
    pl.semaphore_wait(pltpu.get_barrier_semaphore(), count)


def exchange(axis, size, source, slots, send, recv):
    me = lax.axis_index(axis)
    copies = []
    for k in range(1, size):
        peer = lax.rem(me + k, size)
        copy = pltpu.make_async_remote_copy(
            src_ref=source(peer),
            dst_ref=slots.at[me],
            send_sem=send.at[k],
            recv_sem=recv.at[k],
            device_id={axis: peer},
            device_id_type=MESH,
        )
        copy.start()
        copies.append(copy)
    return copies


def landed(copies):
    for copy in copies:
        copy.wait_recv()


def gone(copies):
    for copy in copies:
        copy.wait_send()


def sems(*sizes):
    return [pltpu.SemaphoreType.DMA((size,)) for size in sizes for _ in range(2)]


def split(wide):
    high = wide.astype(bf16)
    return high, (wide - high.astype(f32)).astype(bf16)


def dot_nt(left, right):
    return lax.dot_general(left, right, (((1,), (1,)), ((), ())), preferred_element_type=f32)


def dot(left, right):
    return jnp.dot(left, right, preferred_element_type=f32)


def main_kernel(n, nb, part, level_ref, wave_ref, noise_ref, gain_real, gain_fake, *refs):
    big, refs = refs[:16], refs[16:]
    (difference_ref, norm_ref, weight_ref), refs = refs[:3], refs[3:]
    held, refs = refs[:16], refs[16:]
    (load_sem, patches, parts, modul, fold, gate_fold, gram, inner, stack, qkv, squares,
     square_parts, keys, terms, term_parts, gap, gaps, noisy_ref, share_ref, columns_held, rounded,
     all_rounded, mixed, quarters, merged, grad) = refs[:26]
    sem = refs[26:]
    me = lax.axis_index("tm")
    mine = lax.axis_index("batch")
    core, chip = lax.rem(me, 2), lax.div(me, 2)
    chips = n // 2
    patch_rows, frame = noisy_ref.shape
    level = level_ref[0, 0]
    tokens = n * frame
    width = held[0].shape[1]
    chunks = width // part
    loads = []
    for i, (source, target) in enumerate(zip(big, held)):
        loads.append(pltpu.make_async_copy(source, target, load_sem.at[i]))
    for i in (13, 12, 14, 15, *range(12)):
        loads[i].start()
    nets = [held[6 * i : 6 * i + 6] for i in (0, 1)]
    hidden = held[12]

    hail({"tm": n, "batch": nb})
    loads[13].wait()
    loads[12].wait()
    made = dot_nt(held[13][...], hidden[...]).astype(bf16).astype(f32)
    noisy = ((1.0 - level) * made + level * noise_ref[...].astype(f32)).astype(bf16)
    noisy_ref[...] = noisy
    noisy = noisy.astype(f32)
    for i in (0, 1):
        loads[14 + i].wait()
        for j in range(3):
            share = dot(wave_ref[...], held[14 + i][j])
            for s in range(n):
                if s < chunks:
                    row = share[:1, s * part : (s + 1) * part]
                else:
                    row = jnp.zeros((1, part), f32)
                share_ref[s, 3 * i + j : 3 * i + j + 1] = row
    meet({"tm": n, "batch": nb})
    scatter = exchange("tm", n, lambda peer: share_ref.at[peer], parts, sem[0], sem[1])
    spread = exchange("tm", n, lambda peer: noisy_ref, patches, sem[2], sem[3])
    parts[me] = share_ref[me]
    patches[me] = noisy_ref[...]
    landed(scatter)
    modul[me] = jnp.sum(parts[...], axis=0)
    collect = exchange("tm", n, lambda peer: modul.at[me], modul, sem[4], sem[5])

    def columns(s):
        return pl.ds(pl.multiple_of(s * part, 128), part)

    def own_columns(peer):
        return hidden.at[:, columns(lax.rem(peer, chunks))]

    pass_hidden = exchange("tm", n, own_columns, columns_held, sem[10], sem[11])
    columns_held[me] = hidden[:, columns(lax.rem(me, chunks))]

    means = []
    for i, (embed, proj, query, key, value, out) in enumerate(nets):
        loads[6 * i].wait()
        loads[6 * i + 1].wait()
        mean = jnp.sum(embed[...].astype(f32), axis=1, keepdims=True) / width
        means.append(mean)
        gram[i] = jnp.zeros(gram.shape[1:], f32)
        inner[i] = jnp.zeros(inner.shape[1:], f32)

        def gram_step(s, carry):
            table = embed[:, columns(s)]
            high, low = split(table.astype(f32) - mean)
            own = dot_nt(high, high)
            cross = dot_nt(high, low)
            gram[i] += own + cross + cross.T
            inner[i] += dot_nt(proj[:, columns(s)], table)
            return carry

        lax.fori_loop(0, chunks, gram_step, 0)

    landed(spread)
    kin = 2 * patch_rows
    for s in range(n):
        at = slice(s * frame, (s + 1) * frame)
        now = patches[s]
        before = patches[s - 1] if s else jnp.zeros_like(now)
        both = jnp.concatenate([now, before], axis=0)
        stack[:kin, at] = both
        stack[kin:, at] = both
    landed(collect)

    head = qkv.shape[1] // 3
    for i, (embed, proj, query, key, value, out) in enumerate(nets):
        for j in range(2, 6):
            loads[6 * i + j].wait()
        mean = means[i]
        fold[...] = jnp.zeros_like(fold)
        gate_fold[i] = jnp.zeros(gate_fold.shape[1:], f32)

        def fold_step(s, carry):
            at = columns(s)
            rows = modul[s]
            shift, scale, gate = (rows[3 * i + j : 3 * i + j + 1] for j in range(3))
            high, low = split((embed[:, at].astype(f32) - mean) * (1.0 + scale))
            shift_high, shift_low = split(jnp.broadcast_to(shift, (16, part)))
            left = jnp.concatenate([high, low, shift_high, shift_low], axis=0)
            right = jnp.concatenate([query[at, :], key[at, :], value[at, :]], axis=1)
            fold[...] += dot(left, right)
            high, low = split(proj[:, at].astype(f32) * gate)
            gate_fold[i] += dot_nt(jnp.concatenate([high, low], axis=0), out[:, at])
            return carry

        lax.fori_loop(0, chunks, fold_step, 0)
        folded = (fold[:kin] + fold[kin : 2 * kin]).T
        offset = (fold[2 * kin : 2 * kin + 8] + fold[2 * kin + 16 : 2 * kin + 24]).T[:, :1]
        gram_pair = jnp.concatenate(split(gram[i] / width), axis=1)
        fold_pair = jnp.concatenate(split(folded), axis=1)

        for s in range(n):
            at = slice(s * frame, (s + 1) * frame)
            pair = stack[:, at]
            variance = jnp.sum(pair[:kin].astype(f32) * dot(gram_pair, pair), axis=0, keepdims=True)
            rscale = lax.rsqrt(jnp.maximum(variance, 0.0) + norm_floor)
            full = dot(fold_pair, pair) * rscale + offset
            qkv[i, :, at] = full
            for j in range(2):
                rows = full[j * head : (j + 1) * head]
                squares[2 * i + j : 2 * i + j + 1, at] = jnp.sum(rows * rows, axis=0, keepdims=True)

    sums = exchange("tm", n, lambda peer: squares, square_parts, sem[6], sem[7])
    square_parts[me] = squares[...]
    landed(sums)
    inverse = lax.rsqrt(jnp.sum(square_parts[...], axis=0) / (head * n) + norm_floor)

    block = 2 * frame
    groups = min(4, tokens // block)
    gains = [ref[0:1, :] * ref[1:2, :] for ref in (gain_real, gain_fake)]
    per_group = tokens // block // groups
    for i in range(2):
        for s in range(n):
            at = slice(s * frame, (s + 1) * frame)
            gained = qkv[i, head : 2 * head, at] * inverse[2 * i + 1 : 2 * i + 2, at]
            keys[i, at, :] = (gained.T * gains[i]).astype(bf16)
            qkv[i, :head, at] = qkv[i, :head, at] * inverse[2 * i : 2 * i + 1, at]
    fold_outs = [
        (gate_fold[i, :patch_rows] + gate_fold[i, patch_rows:]).astype(bf16) for i in range(2)
    ]
    for group in range(groups):
        length = (group + 1) * per_group * block

        def block_step(b, carry):
            at = pl.ds(pl.multiple_of(b * block, block), block)
            for i in range(2):
                query = qkv[i, :head, at].astype(bf16)
                scores = dot(keys[i, :length], query)
                low = (length - per_group * block)
                key_frame = (lax.broadcasted_iota(jnp.int32, (length - low, block), 0) + low) // frame
                query_frame = (
                    lax.broadcasted_iota(jnp.int32, (length - low, block), 1) + b * block
                ) // frame
                edge = jnp.where(key_frame <= query_frame, scores[low:], -1e30)
                if low:
                    scores = jnp.concatenate([scores[:low], edge], axis=0)
                else:
                    scores = edge
                peak = jnp.max(scores, axis=0, keepdims=True)
                powers = jnp.exp((scores - peak) * (1.0 / math.sqrt(HD)))
                total = jnp.sum(powers, axis=0, keepdims=True)
                values = qkv[i, 2 * head :, :length].astype(bf16)
                attended = dot(values, powers.astype(bf16)) / total
                term = dot(fold_outs[i], attended.astype(bf16)).astype(bf16)
                for j in range(2):
                    terms[2 * b + j, i * patch_rows : (i + 1) * patch_rows] = term[
                        :, j * frame : (j + 1) * frame
                    ]
            return carry

        if per_group == 1:
            block_step(group, 0)
        else:
            lax.fori_loop(group * per_group, (group + 1) * per_group, block_step, 0)

    give = exchange("tm", n, lambda peer: terms.at[peer], term_parts, sem[8], sem[9])
    term_parts[me] = terms[me]
    own = stack[:, pl.ds(pl.multiple_of(me * frame, frame), frame)]
    direct = [dot(jnp.concatenate(split(inner[i]), axis=1), own) for i in range(2)]
    landed(give)
    summed = jnp.sum(term_parts[...].astype(f32), axis=0)
    pred_real = noisy - level * (summed[:patch_rows] + direct[0])
    pred_fake = noisy - level * (summed[patch_rows:] + direct[1])
    difference = pred_fake - pred_real
    distance = jnp.abs(made - pred_real)
    distance = jnp.sum(jnp.sum(distance, axis=0, keepdims=True), axis=1, keepdims=True)
    gap[...] = jnp.broadcast_to(distance, gap.shape)
    rounded[...] = difference.astype(bf16)
    difference_copies = exchange("tm", n, lambda peer: rounded, all_rounded, sem[12], sem[13])
    gap_copies = exchange("tm", n, lambda peer: gap, gaps, sem[14], sem[15])
    gaps[me] = gap[...]
    all_rounded[me] = rounded[...]
    landed(pass_hidden)
    landed(difference_copies)
    total = dot(all_rounded[0], columns_held[0])
    for s in range(1, n):
        total = total + dot(all_rounded[s], columns_held[s])
    landed(gap_copies)
    normalizer = jnp.maximum(jnp.sum(gaps[...], axis=0) / (patch_rows * tokens), gap_floor)
    norm_ref[...] = normalizer
    difference_ref[...] = difference / normalizer[:1, :1]
    total = total / normalizer[:1, :1] / math.sqrt(nb * tokens)
    mixed[...] = total.reshape(mixed.shape).astype(bf16)
    across = exchange("batch", nb, lambda peer: mixed.at[peer], quarters, sem[16], sem[17])
    quarters[mine] = mixed[mine]
    landed(across)
    merged[mine] = jnp.sum(quarters[...].astype(f32), axis=0).astype(bf16)
    back = exchange("batch", nb, lambda peer: merged.at[mine], merged, sem[18], sem[19])

    grad[core, chip, mine] = merged[mine]
    chain = []

    def to_chips(piece, k):
        copies = []
        for hop in range(1, chips):
            peer = lax.rem(chip + hop, chips)
            copy = pltpu.make_async_remote_copy(
                src_ref=merged.at[piece],
                dst_ref=grad.at[core, chip, piece],
                send_sem=sem[20].at[k * chips + hop],
                recv_sem=sem[21].at[k * chips + hop],
                device_id={"tm": 2 * peer + core},
                device_id_type=MESH,
            )
            copy.start()
            copies.append(copy)
        return copies

    chain.append(to_chips(mine, 0))
    for k in range(1, nb):
        back[k - 1].wait_recv()
        piece = lax.rem(mine + nb - k, nb)
        grad[core, chip, piece] = merged[piece]
        chain.append(to_chips(piece, k))

    def to_partner(at, hop):
        copy = pltpu.make_async_remote_copy(
            src_ref=grad.at[core, at],
            dst_ref=grad.at[core, at],
            send_sem=sem[22].at[hop],
            recv_sem=sem[23].at[hop],
            device_id={"tm": me + 1 - 2 * core},
            device_id_type=MESH,
        )
        copy.start()
        return copy

    shares = [to_partner(chip, 0)]
    for hop in range(1, chips):
        for copies in chain:
            copies[hop - 1].wait_recv()
        shares.append(to_partner(lax.rem(chip + chips - hop, chips), hop))
    landed(shares)
    for s in range(chunks):
        piece = grad[s % 2, s // 2]
        weight_ref[:, s * part : (s + 1) * part] = piece.reshape(patch_rows, part)
    for copies in (
        scatter, spread, collect, pass_hidden, sums, give, difference_copies, gap_copies,
        across, back, *chain, shares,
    ):
        gone(copies)


def sinusoid(time_step):
    half_freq = FREQ // 2
    frequency = jnp.exp(-math.log(10000.0) * jnp.arange(half_freq, dtype=jnp.float32) / half_freq)
    angles = time_step.astype(jnp.float32) * frequency
    return jnp.concatenate([jnp.cos(angles), jnp.sin(angles)]).astype(jnp.bfloat16)


def per_device(
    hidden_states,
    gen_weight,
    noise_field,
    timesteps,
    embed_real,
    time_real,
    query_real,
    key_real,
    value_real,
    out_real,
    gain_real,
    proj_real,
    embed_fake,
    time_fake,
    query_fake,
    key_fake,
    value_fake,
    out_fake,
    gain_fake,
    proj_fake,
):
    devices = lax.axis_size("tm")
    frame_tokens = hidden_states.shape[1]
    tokens = frame_tokens * devices
    patch_rows = gen_weight.shape[0]
    time_step = timesteps[0]
    level_raw = time_step.astype(jnp.float32) / 1000.0
    noise_level = 5.0 * level_raw / (1.0 + 4.0 * level_raw)
    sinus_wave = sinusoid(time_step)
    freq_rows = time_real.shape[0]
    own_wave = lax.dynamic_slice_in_dim(sinus_wave, lax.axis_index("tm") * freq_rows, freq_rows, 0)
    model_width = hidden_states.shape[2]
    batches = lax.axis_size("batch")
    part = -(-model_width // (devices * 128)) * 128
    while model_width % part:
        part += 128
    n, chips, quarter, head = devices, devices // 2, patch_rows // batches, query_real.shape[1]
    kin = 2 * patch_rows
    big = (
        embed_real, proj_real, query_real, key_real, value_real, out_real,
        embed_fake, proj_fake, query_fake, key_fake, value_fake, out_fake,
        hidden_states[0], gen_weight,
        time_real.transpose(1, 0, 2), time_fake.transpose(1, 0, 2),
    )
    vm = pltpu.VMEM
    scratch = [
        *[vm(array.shape, array.dtype) for array in big],
        pltpu.SemaphoreType.DMA((len(big),)),
        vm((n, patch_rows, frame_tokens), bf16),
        vm((n, 6, part), f32),
        vm((n, 6, part), f32),
        vm((2 * kin + 32, 3 * head), f32),
        vm((2, kin, head), f32),
        vm((2, kin, kin), f32),
        vm((2, patch_rows, kin), f32),
        vm((2 * kin, tokens), bf16),
        vm((2, 3 * head, tokens), f32),
        vm((4, tokens), f32),
        vm((n, 4, tokens), f32),
        vm((2, tokens, head), bf16),
        vm((n, kin, frame_tokens), bf16),
        vm((n, kin, frame_tokens), bf16),
        vm((8, 128), f32),
        vm((n, 8, 128), f32),
        vm((patch_rows, frame_tokens), bf16),
        vm((n, 6, part), f32),
        vm((n, frame_tokens, part), bf16),
        vm((patch_rows, frame_tokens), bf16),
        vm((n, patch_rows, frame_tokens), bf16),
        vm((batches, quarter, part), bf16),
        vm((batches, quarter, part), bf16),
        vm((batches, quarter, part), bf16),
        vm((2, chips, batches, quarter, part), bf16),
        *sems(n, n, n, n, n, n, n, n, batches, batches, batches * chips, chips),
    ]
    vmem = pl.BlockSpec(memory_space=pltpu.VMEM)
    difference, norm, weight_grad = pl.pallas_call(
        functools.partial(main_kernel, devices, batches, part),
        out_shape=[
            jax.ShapeDtypeStruct((patch_rows, frame_tokens), f32),
            jax.ShapeDtypeStruct((8, 128), f32),
            jax.ShapeDtypeStruct((patch_rows, model_width), bf16),
        ],
        in_specs=[pl.BlockSpec(memory_space=pltpu.SMEM)] + [vmem] * 4 + [pl.BlockSpec(memory_space=pl.ANY)] * len(big),
        out_specs=[vmem] * 3,
        scratch_shapes=scratch,
        compiler_params=pltpu.CompilerParams(
            collective_id=0, has_side_effects=True, vmem_limit_bytes=60 * 1024 * 1024
        ),
    )(
        noise_level.reshape(1, 1),
        jnp.broadcast_to(own_wave, (16, freq_rows)),
        noise_field[0],
        gain_real,
        gain_fake,
        *big,
    )
    return (difference[None], weight_grad.astype(f32))


def solution(mesh):
    in_specs = (
        P("batch", "tm", None),
        P(),
        P("batch", None, "tm"),
        P("batch"),
        P(),
        P("tm", None, None),
        P(None, "tm"),
        P(None, "tm"),
        P(None, "tm"),
        P("tm", None),
        P(None, "tm"),
        P(),
        P(),
        P("tm", None, None),
        P(None, "tm"),
        P(None, "tm"),
        P(None, "tm"),
        P("tm", None),
        P(None, "tm"),
        P(),
    )
    out_specs = (P("batch", None, "tm"), P())
    return jax.shard_map(
        per_device, mesh=mesh, in_specs=in_specs, out_specs=out_specs, check_vma=False
    )
```
